256 devices in a mesh: dp: 32 (over x, z), expert: 8 (over y, core).
Axes of the slice: x: 4, y: 4, z: 8, core: 2. Of those that a mesh axis runs over, the one named last changes fastest.
Arguments:
- tokens: bfloat16 [32768, 2048], P(('dp', 'expert')), may hold values from -6 to 6
- expert_ids: int32 [32768, 8], P(('dp', 'expert')), may hold values from 0 to 127, all different within a row
- route_probs: float32 [32768, 8], P(('dp', 'expert')), may hold values from 0.05 to 1
- shard_limit: int32 [256, 128], P(('dp', 'expert')), may hold values from 4 to 8
- gate_proj: bfloat16 [256, 2048, 384], P(('dp', 'expert')), may hold values from -0.125 to 0.125
- up_proj: bfloat16 [256, 2048, 384], P(('dp', 'expert')), may hold values from -0.125 to 0.125
- down_proj: bfloat16 [256, 384, 2048], P(('dp', 'expert')), may hold values from -0.21875 to 0.21875
Outputs:
- mixed_out: bfloat16 [32768, 2048], P(('dp', 'expert'))
The draws below stay inside these ranges and needn't reach their ends.
Inputs may be any that keep to these rules, and one draw needn't show every extreme that they name: `expert_ids`: each row names 8 different experts.
All inputs are finite; a program needn't handle non-finite values.
Results may differ from the reference program's by a relative error of at most 0.0095.
Values may be sent and summed in bfloat16 or wider, within the bound.
No kernel may reach another device: no remote copies, remote signals or barrier semaphores. Data moves between devices by JAX's collectives and lax.ppermute only.
A program may use at most 64 MiB of HBM per device.

```python
import math
import jax
import jax.numpy as jnp
from jax import lax

D = 2048
FF = 768
TOP = 8
TOK_DEV = 128
EXPERTS = 128
SHARDS = 256
TOKENS = 32768
CAP = 8
COL_CAP = 128
N_DP = 32
N_EXPERT = 8


def draw_shard_limit(key, part):
    key_base = jax.random.fold_in(key, 11)
    key_full = jax.random.fold_in(key, 12)
    drawn_base = jax.random.randint(key_base, (SHARDS, EXPERTS), CAP // 2, CAP + 1)
    full_mark = jax.random.randint(key_full, (SHARDS, EXPERTS), 0, 2)
    return jnp.where(full_mark == 1, CAP, drawn_base).astype(jnp.int32)


def block_levels(key, extent, split, least, largest):
    factor_of = 1.0
    for dim, parts in split:
        heights = jax.random.uniform(jax.random.fold_in(jax.random.fold_in(key, 6), dim), (parts,), jnp.float32, least / len(split), largest / len(split))
        factor_of = factor_of * jnp.repeat(jnp.exp(heights), extent[dim] // parts).reshape((-1,) + (1,) * (len(extent) - 1 - dim))
    return factor_of


def choose_distinct(own_key, rows, number_of, top, lift):
    sequence = jax.random.permutation(jax.random.fold_in(own_key, 1), number_of)
    boost = sequence
    for power in range(3):
        boost = boost * boost // number_of
    boost = boost * lift // number_of
    lots = jax.random.randint(jax.random.fold_in(own_key, 2), (rows, number_of), 0, 4096) + boost
    sure = jax.random.permutation(jax.random.fold_in(own_key, 3), rows)[jnp.arange(number_of) % rows]
    lots = jnp.where(jnp.arange(rows)[:, None] == sure[None, :], 1 << 14, lots)
    merit = lots * number_of + jnp.arange(number_of)
    return lax.top_k(merit.astype(jnp.int32), top)[1].astype(jnp.int32)


def noise(own_key, shape, spread, most, split=(), held_as=jnp.bfloat16):
    factor_of = block_levels(own_key, shape, split, -0.22, 0.18) if split else 1.0
    values = jax.random.normal(own_key, shape, jnp.float32) * spread * factor_of
    return jnp.minimum(jnp.maximum(values, -most), most).astype(held_as)


def setup_inputs(seed: int = 0) -> dict:
    keys = jax.random.split(jax.random.key(seed), 8)
    return {
        "tokens": noise(keys[0], (TOKENS, D), 1.0, 6.0, ((0, 256),)),
        "expert_ids": choose_distinct(keys[1], TOKENS, EXPERTS, TOP, 1024),
        "route_probs": jnp.clip(jnp.exp(math.log(1.0) - 2.9957323 * jax.random.uniform(keys[2], (TOKENS, TOP), jnp.float32) ** block_levels(keys[2], (TOKENS, TOP), ((0, 256),), -0.2, 0.2)), 0.05, 1.0),
        "shard_limit": draw_shard_limit(jax.random.fold_in(keys[7], 71), 0),
        "gate_proj": noise(keys[4], (2 * EXPERTS, D, FF // 2), D ** -0.5, 0.125, ((0, 256),)),
        "up_proj": noise(keys[5], (2 * EXPERTS, D, FF // 2), D ** -0.5, 0.125, ((0, 256),)),
        "down_proj": noise(keys[6], (2 * EXPERTS, FF // 2, D), FF ** -0.5, 0.21875, ((0, 256),)),
    }


def half_pair(rows_in, gate_pair, up_pair, down_pair):
    partials = []
    for half_index in range(2):
        gate_val = jnp.dot(rows_in, gate_pair[half_index], preferred_element_type=jnp.float32)
        up_val = jnp.dot(rows_in, up_pair[half_index], preferred_element_type=jnp.float32)
        hidden = (jax.nn.silu(gate_val) * up_val).astype(jnp.bfloat16)
        partials.append(jnp.dot(hidden, down_pair[half_index], preferred_element_type=jnp.float32).astype(jnp.bfloat16))
    return (partials[0].astype(jnp.float32) + partials[1].astype(jnp.float32)).astype(jnp.bfloat16)


def expert_apply(packed):
    return half_pair(packed[0], packed[1], packed[2], packed[3])


def reference(tokens, expert_ids, route_probs, shard_limit, gate_proj, up_proj, down_proj):
    shards = N_DP * N_EXPERT
    route_ids = expert_ids.reshape(shards, TOK_DEV * TOP)
    onehot = (route_ids[:, :, None] == jnp.arange(EXPERTS, dtype=jnp.int32)[None, None, :]).astype(jnp.int32)
    before = (jnp.cumsum(onehot, axis=1) - onehot).astype(jnp.int32)
    slot_rank = jnp.sum(before * onehot, axis=2).astype(jnp.int32)
    expert_count = jnp.sum(onehot, axis=1).astype(jnp.int32)
    kept_count = jnp.minimum(expert_count, shard_limit)
    count_grid = kept_count.reshape(N_DP, N_EXPERT, EXPERTS)
    offset = (jnp.cumsum(count_grid, axis=0) - count_grid).astype(jnp.int32).reshape(shards, EXPERTS)
    limit_each = jnp.take_along_axis(shard_limit, route_ids, axis=1)
    offset_each = jnp.take_along_axis(offset, route_ids, axis=1)
    slot_global = offset_each + slot_rank
    kept_mask = (slot_rank < limit_each) & (slot_global < COL_CAP)
    column = (jnp.arange(shards, dtype=jnp.int32) % N_EXPERT)[:, None]
    per_expert = N_EXPERT * COL_CAP
    total_slots = EXPERTS * per_expert
    target = jnp.where(kept_mask, route_ids * per_expert + column * COL_CAP + slot_global, total_slots).astype(jnp.int32)
    target = target.reshape(shards * TOK_DEV, TOP)
    kept_rows = kept_mask.reshape(shards * TOK_DEV, TOP)
    buffers = jnp.zeros((total_slots, D), jnp.bfloat16)
    for choice_num in range(TOP):
        buffers = buffers.at[target[:, choice_num]].set(tokens, mode="drop")
    buffers = buffers.reshape(EXPERTS, per_expert, D)
    expert_rows = lax.map(expert_apply, (buffers, gate_proj.reshape(EXPERTS, 2, D, FF // 2), up_proj.reshape(EXPERTS, 2, D, FF // 2), down_proj.reshape(EXPERTS, 2, FF // 2, D)))
    flat_rows = expert_rows.reshape(total_slots, D)
    total = jnp.zeros((shards * TOK_DEV, D), jnp.float32)
    for choice_num in range(TOP):
        index_now = jnp.minimum(target[:, choice_num], total_slots - 1)
        fetched = flat_rows[index_now].astype(jnp.float32)
        weight = route_probs[:, choice_num] * kept_rows[:, choice_num].astype(jnp.float32)
        total = total + weight[:, None] * fetched
    return total.astype(jnp.bfloat16)
```

```python
import jax
import jax.numpy as jnp
import numpy as np
from jax import lax
from jax.sharding import Mesh, PartitionSpec as P

NX, NZ, NY, NC = 4, 8, 4, 2
CAP = 8
COL_CAP = 128


def shift(block, axis, by):
    n = lax.axis_size(axis)
    return lax.ppermute(block, axis, [(i, (i + by) % n) for i in range(n)])


def slot_tables(expert_ids, route_probs, limits):
    toks = expert_ids.shape[0]
    lane = np.arange(NZ * NX * NY * CAP)
    slot = lane % CAP
    ep = lane // CAP
    expert = (ep // NY % NX) * (NZ * NY) + (ep // (NX * NY)) * NY + ep % NY
    expert = jnp.asarray(expert, jnp.int32)[None, :]
    slot = jnp.asarray(slot, jnp.float32)[None, :]
    pick = (jnp.arange(limits.shape[0], dtype=jnp.int32)[:, None] == expert).astype(jnp.bfloat16)
    lim = jnp.dot(limits[None, :].astype(jnp.bfloat16), pick, preferred_element_type=jnp.float32)
    hit = jnp.zeros((toks, lane.size), jnp.float32)
    weight = jnp.zeros((toks, lane.size), jnp.float32)
    for k in range(expert_ids.shape[1]):
        same = expert_ids[:, k : k + 1] == expert
        hit = hit + same.astype(jnp.float32)
        weight = weight + jnp.where(same, route_probs[:, k : k + 1], 0.0)
    row = jnp.arange(toks, dtype=jnp.int32)
    below = (row[:, None] > row[None, :]).astype(jnp.bfloat16)
    rank = jnp.dot(below, hit.astype(jnp.bfloat16), preferred_element_type=jnp.float32)
    here = (hit > 0) & (rank == slot) & (rank < lim)
    tok = jnp.sum(jnp.where(here, (row[:, None] + 1).astype(jnp.float32), 0.0), axis=0) - 1.0
    wgt = jnp.sum(jnp.where(here, weight, 0.0), axis=0)
    count = jnp.minimum(jnp.sum(hit, axis=0), lim[0])
    table = jnp.stack([tok, wgt, count])
    return jnp.swapaxes(table.reshape(3, NZ, NX * NY * CAP), 0, 1)


def on_device(tokens, expert_ids, route_probs, shard_limit, gate_proj, up_proj, down_proj):
    toks, width = tokens.shape
    half = width // 2
    f32, bf16 = jnp.float32, jnp.bfloat16
    z = lax.axis_index("z")
    x = lax.axis_index("x")

    fwd, bwd = [tokens], [tokens]
    for _ in range(3):
        fwd.append(shift(fwd[-1], "z", 1))
        bwd.append(shift(bwd[-1], "z", -1))
    far = jnp.concatenate([shift(fwd[3][:, :half], "z", 1), shift(bwd[3][:, half:], "z", -1)], 1)

    gate = jnp.concatenate([gate_proj[0], shift(gate_proj[0], "c", 1)], axis=1)
    up = jnp.concatenate([up_proj[0], shift(up_proj[0], "c", 1)], axis=1)
    down = jnp.concatenate([down_proj[0], shift(down_proj[0], "c", 1)], axis=0)

    table = slot_tables(expert_ids, route_probs, shard_limit[0])
    seen = lax.all_to_all(table, "z", 0, 0, tiled=True)
    lanes = table.shape[2]
    counts = seen[:, 2]
    line = jnp.sum(counts, axis=0)
    others = lax.all_to_all(jnp.broadcast_to(line, (NX, lanes)), "x", 0, 0, tiled=True)
    base = jnp.sum(jnp.where(jnp.arange(NX)[:, None] < x, others, 0.0), axis=0)
    slot = jnp.asarray(np.arange(lanes) % CAP, f32)

    def placed(src):
        before = jnp.sum(jnp.where(jnp.arange(NZ)[:, None] < src, counts, 0.0), axis=0)
        return base + before + slot < COL_CAP

    def tok_of(src):
        return lax.dynamic_index_in_dim(seen[:, 0], src, 0, keepdims=False)

    def wgt_of(src):
        w = lax.dynamic_index_in_dim(seen[:, 1], src, 0, keepdims=False)
        return jnp.where(placed(src), w, 0.0)

    own_tok = lax.dynamic_index_in_dim(table[:, 0], z, 0, keepdims=False)
    groups = [
        ((0,), tokens),
        ((-1, 1), None),
        ((-2, 2), None),
        ((-3, 3), None),
        ((4,), far),
    ]

    def by_slot(rows):
        n = len(rows)
        return jnp.stack([r.reshape(NX * NY, CAP) for r in rows], 1).reshape(-1)

    outs = []
    for g, (offs, block) in enumerate(groups):
        n = len(offs)
        if block is None:
            block = jnp.concatenate([fwd[g], bwd[g]], axis=0)
        idx = []
        for s, off in enumerate(offs):
            t = own_tok if off == 0 else tok_of((z + off) % NZ)
            idx.append(jnp.where(t < 0, -1.0, t + s * toks))
        idx = by_slot(idx)
        pos = jnp.arange(n * toks, dtype=jnp.int32).astype(f32)
        send = jnp.dot(
            (idx[:, None] == pos[None, :]).astype(bf16), block, preferred_element_type=f32
        ).astype(bf16)
        got = lax.all_to_all(
            send.reshape(NX * NY, n * CAP, width), ("x", "y"), 0, 0, tiled=True
        ).reshape(-1, width)
        a = jnp.dot(got, gate, preferred_element_type=f32)
        b = jnp.dot(got, up, preferred_element_type=f32)
        hidden = (jax.nn.silu(a) * b).astype(bf16)
        res = jnp.dot(hidden, down, preferred_element_type=f32).astype(bf16)
        outs.append((idx, res))

    to_fwd = to_bwd = None
    mixed = None
    for g in (4, 3, 2, 1, 0):
        offs = groups[g][0]
        n = len(offs)
        idx, res = outs[g]
        back = lax.all_to_all(
            res.reshape(NX * NY, n * CAP, width), ("x", "y"), 0, 0, tiled=True
        ).reshape(-1, width)
        w = by_slot([wgt_of((z + off) % NZ) for off in offs])
        pos = jnp.arange(n * toks, dtype=jnp.int32).astype(f32)
        mix = jnp.where(idx[None, :] == pos[:, None], w[None, :], 0.0).astype(bf16)
        part = jnp.dot(mix, back, preferred_element_type=f32)
        if g == 4:
            to_bwd = shift(part[:, :half].astype(bf16), "z", -1)
            to_fwd = shift(part[:, half:].astype(bf16), "z", 1)
        elif g == 3:
            lo, hi = part[:toks], part[toks:]
            lo = jnp.concatenate([lo[:, :half] + to_bwd.astype(f32), lo[:, half:]], 1)
            hi = jnp.concatenate([hi[:, :half], hi[:, half:] + to_fwd.astype(f32)], 1)
            to_bwd = shift(lo.astype(bf16), "z", -1)
            to_fwd = shift(hi.astype(bf16), "z", 1)
        elif g > 0:
            to_bwd = shift((part[:toks] + to_bwd.astype(f32)).astype(bf16), "z", -1)
            to_fwd = shift((part[toks:] + to_fwd.astype(f32)).astype(bf16), "z", 1)
        else:
            mixed = part + to_bwd.astype(f32) + to_fwd.astype(f32)
    return mixed.astype(bf16)


def solution(mesh):
    fine = Mesh(mesh.devices.reshape(NX, NZ, NY, NC), ("x", "z", "y", "c"))
    spec = P(("x", "z", "y", "c"))
    return jax.shard_map(on_device, mesh=fine, in_specs=(spec,) * 7, out_specs=spec, check_vma=False)
```

```python
import functools

import jax
import jax.numpy as jnp
import numpy as np
from jax import lax
from jax.experimental import pallas as pl
from jax.experimental.pallas import tpu as pltpu
from jax.sharding import Mesh, PartitionSpec as P

NX, NZ, NY, NC = 4, 8, 4, 2
CAP = 8
COL_CAP = 128
META = 8
LANES = NX * NY * CAP
F32, BF16 = jnp.float32, jnp.bfloat16
VMEM = pl.BlockSpec(memory_space=pltpu.VMEM)
SMEM = pl.BlockSpec(memory_space=pltpu.SMEM)


def shift(block, axis, by):
    n = lax.axis_size(axis)
    return lax.ppermute(block, axis, [(i, (i + by) % n) for i in range(n)])


def call(body, ins, outs, scratch=(), smem=1):
    outs = pl.pallas_call(
        body,
        out_shape=[jax.ShapeDtypeStruct(s, d) for s, d in outs],
        in_specs=[SMEM] * smem + [VMEM] * (len(ins) - smem),
        out_specs=[VMEM] * len(outs),
        scratch_shapes=list(scratch),
        compiler_params=pltpu.CompilerParams(vmem_limit_bytes=40 * 2**20),
    )(*ins)
    return list(outs)


def tables_body(tok_ref, ids_ref, prob_ref, lim_ref, out_ref):
    toks, half = tok_ref.shape[0], out_ref.shape[1]
    out_ref[:toks, :] = tok_ref[:, half:]
    ids = ids_ref[...].astype(F32).T
    prob = prob_ref[...].T
    lims = lim_ref[...].astype(F32)
    row = lax.broadcasted_iota(jnp.int32, (toks, toks), 0)
    col = lax.broadcasted_iota(jnp.int32, (toks, toks), 1)
    below = (row > col).astype(F32).astype(BF16)

    def plane(zp, carry):
        lane = lax.broadcasted_iota(jnp.int32, (toks, LANES), 1)
        expert = (lane // (NY * CAP)) * (NZ * NY) + zp * NY + lane // CAP % NY
        slot = (lane % CAP).astype(F32)
        pick = (lax.broadcasted_iota(jnp.int32, (toks, LANES), 0) == expert).astype(F32)
        lim = jnp.dot(
            jnp.broadcast_to(lims, (8, toks)).astype(BF16), pick.astype(BF16), preferred_element_type=F32
        )[:1]
        wanted = expert.astype(F32)
        hit = jnp.zeros((toks, LANES), F32)
        weight = jnp.zeros((toks, LANES), F32)
        for k in range(ids.shape[1]):
            same = ids[:, k : k + 1] == wanted
            hit = jnp.where(same, 1.0, hit)
            weight = jnp.where(same, prob[:, k : k + 1], weight)
        rank = jnp.dot(below, hit.astype(BF16), preferred_element_type=F32)
        here = (hit > 0) & (rank == slot) & (rank < lim)
        number = (lax.broadcasted_iota(jnp.int32, (toks, LANES), 0) + 1).astype(F32)
        tok = jnp.sum(jnp.where(here, number, 0.0), axis=0, keepdims=True)
        wgt = jnp.sum(jnp.where(here, weight, 0.0), axis=0, keepdims=True)
        count = jnp.minimum(jnp.sum(hit, axis=0, keepdims=True), lim)
        rows = jnp.concatenate([tok, wgt, count, jnp.zeros((META - 3, LANES), F32)], axis=0)
        out_ref[toks:, pl.ds(pl.multiple_of(zp * LANES, LANES), LANES)] = rows.astype(BF16)
        return carry

    lax.fori_loop(0, NZ, plane, 0)


def relative(row, x, y):
    row = jnp.broadcast_to(row, (8, LANES))
    lane = lax.broadcasted_iota(jnp.int32, row.shape, 1)
    group = NY * CAP
    near = pltpu.roll(row, (2 * LANES - x * group - y * CAP) % LANES, 1)
    wrap = pltpu.roll(row, (2 * LANES + group - x * group - y * CAP) % LANES, 1)
    return jnp.where(lane % group + y * CAP < group, near, wrap)[:1]


def gather_body(n, at_ref, *refs):
    blocks, outs, meta_ref, pick_ref = refs[: 2 * n], refs[2 * n : -2], refs[-2], refs[-1]
    x, y, z = at_ref[0], at_ref[1], at_ref[2]
    toks = 128
    half = blocks[0].shape[1]
    part = NY * CAP
    for s in range(n):
        rows = blocks[2 * s + 1][toks:, pl.ds(pl.multiple_of(z * LANES, LANES), LANES)].astype(F32)
        meta_ref[8 * s : 8 * s + 8, :] = rows
        tok = relative(rows[:1], x, y)
        number = (lax.broadcasted_iota(jnp.int32, (toks, LANES), 0) + 1).astype(F32)
        pick_ref[s * LANES : (s + 1) * LANES, :] = (number == tok).astype(F32).T.astype(BF16)
    chunk = 256

    def step(c, carry):
        cols = pl.ds(pl.multiple_of(c * chunk, chunk), chunk)
        for s in range(n):
            pick = pick_ref[s * LANES : (s + 1) * LANES, :]
            for h in range(2):
                got = jnp.dot(pick, blocks[2 * s + h][:toks, cols], preferred_element_type=F32).astype(BF16)
                to = pl.ds(pl.multiple_of(h * half + c * chunk, chunk), chunk)
                for d in range(NX):
                    outs[d][s * part : (s + 1) * part, to] = got[d * part : (d + 1) * part]
        return carry

    lax.fori_loop(0, half // chunk, step, 0)


def gather(at, blocks, width):
    n = len(blocks) // 2
    outs = [((n * NY * CAP, width), BF16)] * NX + [((8 * n, LANES), F32)]
    return call(
        functools.partial(gather_body, n),
        [at, *blocks],
        outs,
        [pltpu.VMEM((n * LANES, LANES), BF16)],
    )


def regroup_body(n, into, *refs):
    ins, outs = refs[:NX], refs[NX:]
    for d in range(NX):
        for e in range(NY):
            for s in range(n):
                a, b = (s * NY + e) * CAP, (d * n + s) * CAP
                if into:
                    outs[e][b : b + CAP, :] = ins[d][a : a + CAP, :]
                else:
                    outs[d][a : a + CAP, :] = ins[e][b : b + CAP, :]


def regroup(blocks, n, into):
    return call(
        functools.partial(regroup_body, n, into), blocks, [(b.shape, BF16) for b in blocks], smem=0
    )


def ffn_body(gate_ref, up_ref, down_ref, *refs):
    ins, outs, rows_ref, hid_ref = refs[:NY], refs[NY : 2 * NY], refs[-2], refs[-1]
    m = ins[0].shape[0]
    for i, r in enumerate(ins):
        rows_ref[i * m : (i + 1) * m, :] = r[...]
    chunk = 256

    def inner(c, carry):
        cols = pl.ds(pl.multiple_of(c * chunk, chunk), chunk)
        a = jnp.dot(rows_ref[...], gate_ref[:, cols], preferred_element_type=F32)
        b = jnp.dot(rows_ref[...], up_ref[:, cols], preferred_element_type=F32)
        hid_ref[:, cols] = (a / (1.0 + jnp.exp(-a)) * b).astype(BF16)
        return carry

    lax.fori_loop(0, hid_ref.shape[1] // chunk, inner, 0)

    def outer(c, carry):
        cols = pl.ds(pl.multiple_of(c * chunk, chunk), chunk)
        got = jnp.dot(hid_ref[...], down_ref[:, cols], preferred_element_type=F32).astype(BF16)
        for i, o in enumerate(outs):
            o[:, cols] = got[i * m : (i + 1) * m]
        return carry

    lax.fori_loop(0, down_ref.shape[1] // chunk, outer, 0)


def ffn(rows, gate, up, down):
    m, width = rows[0].shape
    return call(
        ffn_body,
        [gate, up, down, *rows],
        [((m, width), BF16)] * NY,
        [pltpu.VMEM((NY * m, width), BF16), pltpu.VMEM((NY * m, gate.shape[1]), BF16)],
        smem=0,
    )


def mix_body(n, nadd, split, at_ref, meta_ref, wgt_ref, *refs):
    backs, adds, outs, mix_ref = refs[:NX], refs[NX : NX + nadd], refs[NX + nadd : -1], refs[-1]
    x, y = at_ref[0], at_ref[1]
    toks = 128
    part = NY * CAP
    half = backs[0].shape[1] // 2
    for s in range(n):
        tok = relative(meta_ref[8 * s : 8 * s + 1, :], x, y)
        wgt = relative(wgt_ref[s : s + 1, :], x, y)
        number = (lax.broadcasted_iota(jnp.int32, (toks, LANES), 0) + 1).astype(F32)
        mix_ref[s * toks : (s + 1) * toks, :] = jnp.where(number == tok, wgt, 0.0).astype(BF16)
    chunk = 256

    def step(c, carry):
        cols = pl.ds(pl.multiple_of(c * chunk, chunk), chunk)
        for s in range(n):
            for h in range(2):
                frm = pl.ds(pl.multiple_of(h * half + c * chunk, chunk), chunk)
                rows = jnp.concatenate([b[s * part : (s + 1) * part, frm] for b in backs], axis=0)
                got = jnp.dot(mix_ref[s * toks : (s + 1) * toks, :], rows, preferred_element_type=F32)
                if split:
                    if nadd == 4:
                        got = got + adds[2 * s + h][:, cols].astype(F32)
                    elif nadd == 2 and h == s:
                        got = got + adds[s][:, cols].astype(F32)
                    outs[2 * s + h][:, cols] = got.astype(BF16)
                else:
                    got = got + (adds[h][:, cols].astype(F32) + adds[2 + h][:, cols].astype(F32))
                    outs[0][:, frm] = got.astype(BF16)
        return carry

    lax.fori_loop(0, half // chunk, step, 0)


def mixing(at, meta, wgt, backs, adds, split):
    n = wgt.shape[0]
    width = backs[0].shape[1]
    outs = [((128, width // 2), BF16)] * (2 * n) if split else [((128, width), BF16)]
    return call(
        functools.partial(mix_body, n, len(adds), split),
        [at, meta, wgt, *backs, *adds],
        outs,
        [pltpu.VMEM((n * 128, LANES), BF16)],
    )


def on_device(tokens, expert_ids, route_probs, shard_limit, gate_proj, up_proj, down_proj):
    toks, width = tokens.shape
    half = width // 2
    x, y, z = (lax.axis_index(a) for a in "xyz")
    at = jnp.stack([x, y, z]).astype(jnp.int32)

    own_a = tokens[:, :half]
    (own_b,) = call(
        tables_body,
        [tokens, expert_ids.T, route_probs.T, shard_limit],
        [((toks + META, half), BF16)],
        smem=0,
    )

    ahead, behind = {0: (own_a, own_b)}, {0: (own_a, own_b)}
    for i in (1, 2, 3, 4):
        fa = shift(ahead[i - 1][0], "z", 1)
        ba = shift(behind[i - 1][0], "z", -1) if i < 4 else None
        bb = shift(behind[i - 1][1], "z", -1)
        fb = shift(ahead[i - 1][1], "z", 1) if i < 4 else None
        ahead[i], behind[i] = (fa, fb), (ba, bb)

    gate = jnp.concatenate([gate_proj[0], shift(gate_proj[0], "c", 1)], axis=1)
    up = jnp.concatenate([up_proj[0], shift(up_proj[0], "c", 1)], axis=1)
    down = jnp.concatenate([down_proj[0], shift(down_proj[0], "c", 1)], axis=0)

    groups = [((0,), (own_a, own_b))]
    groups += [((-i, i), (*ahead[i], *behind[i])) for i in (1, 2, 3)]
    groups += [((4,), (ahead[4][0], behind[4][1]))]

    metas, results = [], []
    for offs, blocks in groups:
        n = len(offs)
        *got, meta = gather(at, blocks, width)
        metas.append(meta)
        got = got[:1] + [shift(got[s], "x", s) for s in (1, 2, 3)]
        got = regroup(got, n, True)
        got = got[:1] + [shift(got[s], "y", s) for s in (1, 2, 3)]
        results.append(ffn(got, gate, up, down))

    offsets = [off for offs, _ in groups for off in offs]
    info = jnp.concatenate(metas, axis=0).reshape(len(offsets), 8, LANES)
    counts = info[:, 2]
    line = jnp.sum(counts, axis=0, keepdims=True)
    base = jnp.zeros_like(line)
    for s in (1, 2, 3):
        base = base + jnp.where(x >= s, shift(line, "x", s), 0.0)
    src = (z + jnp.asarray(offsets, jnp.int32)) % NZ
    earlier = (src[None, :] < src[:, None]).astype(BF16)
    before = jnp.dot(earlier, counts.astype(BF16), preferred_element_type=F32)
    slot = jnp.asarray(np.arange(LANES) % CAP, F32)
    weights = jnp.where(base + before + slot[None, :] < COL_CAP, info[:, 1], 0.0)

    acc = []
    for g in (4, 3, 2, 1, 0):
        n = len(groups[g][0])
        got = results[g]
        got = got[:1] + [shift(got[s], "y", -s) for s in (1, 2, 3)]
        got = regroup(got, n, False)
        got = got[:1] + [shift(got[s], "x", -s) for s in (1, 2, 3)]
        first = sum(len(offs) for offs, _ in groups[:g])
        acc = mixing(at, metas[g], weights[first : first + n], got, acc, g > 0)
        if g == 4:
            acc = [shift(acc[0], "z", -1), shift(acc[1], "z", 1)]
        elif g > 0:
            acc = [shift(p, "z", -1) for p in acc[:2]] + [shift(p, "z", 1) for p in acc[2:]]
    return acc[0]


def solution(mesh):
    fine = Mesh(mesh.devices.reshape(NX, NZ, NY, NC), ("x", "z", "y", "c"))
    spec = P(("x", "z", "y", "c"))

    return jax.shard_map(on_device, mesh=fine, in_specs=(spec,) * 7, out_specs=spec, check_vma=False)
```
